512 devices in a mesh: dp: 128 (over x, y, z_hi, core), rep: 4 (over z_lo).
Axes of the slice: x: 4, y: 4, z: 16 (z_hi: 4, z_lo: 4; z = z_hi * 4 + z_lo), core: 2. Of those that a mesh axis runs over, the one named last changes fastest.
Arguments:
- student_in: bfloat16 [262144, 320], P(('dp', 'rep')), may hold values from -6 to 6
- target_in: bfloat16 [262144, 320], P(('dp', 'rep')), may hold values from -6 to 6
- timesteps: int32 [1024], P(('dp', 'rep')), may hold values from 20 to 999
- student_win: float32 [1280, 320], P('dp'), may hold values from -0.3125 to 0.3125
- student_wout: float32 [640, 320], P('dp'), may hold values from -0.25 to 0.25
- student_wtime: float32 [640, 320], P('dp'), may hold values from -0.25 to 0.25
- student_gain: float32 [320], replicated, may hold values from 0.5 to 1.5
- student_bias: float32 [320], replicated, may hold values from -3 to 3
- target_win: float32 [1280, 320], P('dp'), may hold values from -0.3125 to 0.3125
- target_wout: float32 [640, 320], P('dp'), may hold values from -0.25 to 0.25
- target_wtime: float32 [640, 320], P('dp'), may hold values from -0.25 to 0.25
- target_gain: float32 [320], replicated, may hold values from 0.5 to 1.5
- target_bias: float32 [320], replicated, may hold values from -3 to 3
Outputs:
- grad_win: float32 [1280, 320], P('dp')
- grad_wout: float32 [640, 320], P('dp')
- grad_wtime: float32 [640, 320], P('dp')
- grad_gain: float32 [320], replicated
- grad_bias: float32 [320], replicated
- ema_win: float32 [1280, 320], P('dp')
- ema_wout: float32 [640, 320], P('dp')
- ema_wtime: float32 [640, 320], P('dp')
- ema_gain: float32 [320], replicated
- ema_bias: float32 [320], replicated
The draws below stay inside these ranges and needn't reach their ends.
Inputs may be any that keep to these rules, and one draw needn't show every extreme that they name: `timesteps`: student timestep of each sample; the target is evaluated at 20 steps earlier.
All inputs are finite; a program needn't handle non-finite values.
Results may differ from the reference program's by a relative error of at most 0.004.
The reference program's roundings to bfloat16 on the way (of `time_feat`, `normed_b`, `hidden`, `grad_yb` and `grad_mix`) count: a program that leaves them out, or rounds other values in their place, can miss the bound.
Values may be sent and summed in bfloat16 or wider, within the bound.
A program may use at most 64 MiB of HBM per device.

```python
import math
import jax
import jax.numpy as jnp
from jax import lax

D = 320
FF = 640
TEMB = 640
SKIP = 20
TOK_DEV = 512
SAMPLES = 1024
TOKENS = 262144
N_DP = 128


def set_ends(values, key, least, top_value):
    longest = values.shape.index(max(values.shape))
    spots = []
    for shift in (0, 1):
        where = [jax.random.randint(jax.random.fold_in(key, axis), (), 0, length) for axis, length in enumerate(values.shape)]
        where[longest] = (where[longest] + shift) % values.shape[longest]
        spots.append(tuple(where))
    return values.at[spots[0]].set(least).at[spots[1]].set(top_value)


def levels(stream_key, dims, split, least, largest):
    def one(axis_at, shards_of):
        steps = jax.random.uniform(jax.random.fold_in(jax.random.fold_in(stream_key, 6), axis_at), (shards_of,), jnp.float32, least / len(split), largest / len(split))
        return jnp.repeat(jnp.exp(steps), dims[axis_at] // shards_of).reshape((-1,) + (1,) * (len(dims) - axis_at - 1))

    level = one(*split[0])
    for cut in split[1:]:
        level = level * one(*cut)
    return level


def normal_values(own_key, extent, spread, most, shards=(), kind=jnp.bfloat16):
    values = spread * jax.random.normal(own_key, extent, jnp.float32)
    if shards:
        values = values * levels(own_key, extent, shards, -0.22, 0.18)
    return jnp.clip(values, -most, most).astype(kind)


def setup_inputs(seed: int = 0) -> dict:
    keys = jax.random.split(jax.random.key(seed), 14)
    return {
        "student_in": normal_values(keys[0], (TOKENS, D), 1.0, 6.0, ((0, 512),)),
        "target_in": normal_values(keys[1], (TOKENS, D), 1.0, 6.0, ((0, 512),)),
        "timesteps": set_ends(jax.random.randint(keys[2], (SAMPLES,), SKIP, 1000), jax.random.fold_in(keys[2], 1), SKIP, 999).astype(jnp.int32),
        "student_win": normal_values(keys[3], (2 * FF, D), D ** -0.5, 0.3125, ((0, 128),), jnp.float32),
        "student_wout": normal_values(keys[4], (FF, D), FF ** -0.5, 0.25, ((0, 128),), jnp.float32),
        "student_wtime": normal_values(keys[5], (TEMB, D), TEMB ** -0.5, 0.25, ((0, 128),), jnp.float32),
        "student_gain": jnp.clip(1.0 + 0.1 * jax.random.normal(keys[6], (D,), jnp.float32), 0.5, 1.5),
        "student_bias": normal_values(keys[7], (D,), 0.5, 3.0, (), jnp.float32),
        "target_win": normal_values(keys[8], (2 * FF, D), D ** -0.5, 0.3125, ((0, 128),), jnp.float32),
        "target_wout": normal_values(keys[9], (FF, D), FF ** -0.5, 0.25, ((0, 128),), jnp.float32),
        "target_wtime": normal_values(keys[10], (TEMB, D), TEMB ** -0.5, 0.25, ((0, 128),), jnp.float32),
        "target_gain": jnp.clip(1.0 + 0.1 * jax.random.normal(keys[11], (D,), jnp.float32), 0.5, 1.5),
        "target_bias": normal_values(keys[12], (D,), 0.5, 3.0, (), jnp.float32),
    }


ema_decay = 0.95
learn_rate = 0.05

def sinusoid(step_ids, width):
    half_width = width // 2
    frequency = jnp.exp(-math.log(10000.0) * jnp.arange(half_width, dtype=jnp.float32) / half_width)
    angles = step_ids.astype(jnp.float32)[:, None] * frequency[None, :]
    return jnp.concatenate([jnp.cos(angles), jnp.sin(angles)], axis=1)

def gelu_tanh(value):
    inner = 0.7978845608 * (value + 0.044715 * value * value * value)
    return 0.5 * value * (1.0 + jnp.tanh(inner))

def gelu_slope(value):
    tangent = jnp.tanh(0.7978845608 * (value + 0.044715 * value * value * value))
    return 0.5 * (1.0 + tangent) + 0.5 * value * (1.0 - tangent * tangent) * 0.7978845608 * (1.0 + 0.134145 * value * value)

def contract_last(left, right):
    return lax.dot_general(left, right, (((1,), (1,)), ((), ())), preferred_element_type=jnp.float32)

def contract_first(left, right):
    return lax.dot_general(left, right, (((0,), (0,)), ((), ())), preferred_element_type=jnp.float32)

def forward(tok_rows, step_ids, w_in, w_out, w_time, gain, bias):
    time_feat = jax.nn.silu(sinusoid(step_ids, w_time.shape[0])).astype(jnp.bfloat16)
    embedding = jnp.dot(time_feat, w_time, preferred_element_type=jnp.float32)
    samples = step_ids.shape[0]
    width = tok_rows.shape[1]
    summed = tok_rows.astype(jnp.float32).reshape(samples, -1, width) + embedding[:, None, :]
    summed = summed.reshape(-1, width)
    center = summed - lax.optimization_barrier(jnp.mean(summed, axis=1, keepdims=True))
    inv_std = lax.rsqrt(lax.optimization_barrier(jnp.mean(center * center, axis=1, keepdims=True)) + 1e-05)
    normed = center * inv_std
    normed_b = (normed * gain + bias).astype(jnp.bfloat16)
    mixed = contract_last(normed_b, w_in)
    hidden_count = w_out.shape[0]
    gate_part = mixed[:, :hidden_count]
    up_part = mixed[:, hidden_count:]
    gelu_gate = gelu_tanh(gate_part)
    hidden = (gelu_gate * up_part).astype(jnp.bfloat16)
    output = summed + jnp.dot(hidden, w_out, preferred_element_type=jnp.float32)
    return (output, (time_feat, normed, inv_std, normed_b, gate_part, up_part, gelu_gate, hidden))

def backward(grad_y, saved, w_in, w_out, gain):
    time_feat, normed, inv_std, normed_b, gate_part, up_part, gelu_gate, hidden = saved
    grad_yb = grad_y.astype(jnp.bfloat16)
    grad_h = contract_last(grad_yb, w_out)
    grad_mix = jnp.concatenate([grad_h * up_part * gelu_slope(gate_part), grad_h * gelu_gate], axis=1).astype(jnp.bfloat16)
    grad_z = jnp.dot(grad_mix, w_in, preferred_element_type=jnp.float32)
    grad_gain = lax.optimization_barrier(jnp.sum(grad_z * normed, axis=0))
    grad_bias = lax.optimization_barrier(jnp.sum(grad_z, axis=0))
    grad_n = grad_z * gain
    grad_s = grad_y + inv_std * (grad_n - lax.optimization_barrier(jnp.mean(grad_n, axis=1, keepdims=True)) - normed * lax.optimization_barrier(jnp.mean(grad_n * normed, axis=1, keepdims=True)))
    samples = time_feat.shape[0]
    grad_emb = lax.optimization_barrier(jnp.sum(grad_s.reshape(samples, -1, grad_s.shape[1]), axis=1))
    grad_time = lax.dot_general(time_feat.astype(jnp.float32), grad_emb, (((0,), (0,)), ((), ())), precision=lax.Precision.HIGHEST, preferred_element_type=jnp.float32)
    return (grad_yb, grad_mix, grad_gain, grad_bias, grad_time)

def reference(student_in, target_in, timesteps, student_win, student_wout, student_wtime, student_gain, student_bias, target_win, target_wout, target_wtime, target_gain, target_bias):
    s_in = student_win.astype(jnp.bfloat16)
    s_out = student_wout.astype(jnp.bfloat16)
    s_time = student_wtime.astype(jnp.bfloat16)
    t_in = target_win.astype(jnp.bfloat16)
    t_out = target_wout.astype(jnp.bfloat16)
    t_time = target_wtime.astype(jnp.bfloat16)
    width = student_in.shape[1]
    student_blocks = student_in.reshape(N_DP, -1, width)
    target_blocks = target_in.reshape(N_DP, -1, width)
    step_blocks = timesteps.reshape(N_DP, -1)

    def one_block(carry, block):
        s_rows, t_rows, step_ids = block
        student_out, saved = forward(s_rows, step_ids, s_in, s_out, s_time, student_gain, student_bias)
        target_out, unused = forward(t_rows, step_ids - SKIP, t_in, t_out, t_time, target_gain, target_bias)
        grad_y = (student_out - target_out) / TOK_DEV
        grad_yb, grad_mix, grad_gain, grad_bias, grad_time = backward(grad_y, saved, s_in, s_out, student_gain)
        grad_in = contract_first(grad_mix, saved[3])
        grad_out = contract_first(saved[7], grad_yb)
        totals = (carry[0] + grad_in, carry[1] + grad_out, carry[2] + grad_time, carry[3] + grad_gain, carry[4] + grad_bias)
        return (totals, None)
    start = (jnp.zeros(student_win.shape, jnp.float32), jnp.zeros(student_wout.shape, jnp.float32), jnp.zeros(student_wtime.shape, jnp.float32), jnp.zeros(student_gain.shape, jnp.float32), jnp.zeros(student_bias.shape, jnp.float32))
    totals, unused = lax.scan(one_block, start, (student_blocks, target_blocks, step_blocks))
    grad_win, grad_wout, grad_wtime, grad_gain, grad_bias = totals

    def average(target_p, student_p, grad_p):
        return ema_decay * target_p + (1.0 - ema_decay) * (student_p - learn_rate * grad_p)
    return (grad_win, grad_wout, grad_wtime, grad_gain, grad_bias, average(target_win, student_win, grad_win), average(target_wout, student_wout, grad_wout), average(target_wtime, student_wtime, grad_wtime), average(target_gain, student_gain, grad_gain), average(target_bias, student_bias, grad_bias))
```

```python
import functools
import math

import jax
import jax.numpy as jnp
import numpy as np
from jax import lax
from jax.experimental import pallas as pl
from jax.experimental.pallas import tpu as pltpu
from jax.sharding import Mesh
from jax.sharding import PartitionSpec as P

SKIP = 20
DP = ("x", "y", "zh", "core")
DP_REP = ("x", "y", "zh", "core", "zl")
EMA_DECAY = 0.95
LEARN_RATE = 0.05
F32, BF16 = jnp.float32, jnp.bfloat16
VMEM = pl.BlockSpec(memory_space=pltpu.VMEM)


def here():
    return tuple(lax.axis_index(a) for a in ("x", "y", "zh", "core", "zl"))


def send(src, dst, send_sem, recv_sem, device):
    copy = pltpu.make_async_remote_copy(
        src_ref=src,
        dst_ref=dst,
        send_sem=send_sem,
        recv_sem=recv_sem,
        device_id=device,
        device_id_type=pl.DeviceIdType.MESH,
    )
    copy.start()
    return copy


def greet(device):
    pl.semaphore_signal(
        pltpu.get_barrier_semaphore(), inc=1, device_id=device, device_id_type=pl.DeviceIdType.MESH
    )


class Sender:
    def __init__(self, send_sems, recv_sems):
        self.send_sems, self.recv_sems, self.started = send_sems, recv_sems, []

    def __call__(self, src, dst, device):
        at = len(self.started)
        copy = send(src, dst, self.send_sems.at[at], self.recv_sems.at[at], device)
        self.started.append(copy)
        return copy

    def finish(self):
        for copy in self.started:
            copy.wait_send()


def along(first, k, x, y, c):
    on_x = (1 - c) if first else c
    return {"x": (x + on_x * k) % 4, "y": (y + (1 - on_x) * k) % 4}


def block(k, m, x, y, c):
    return ((x + (1 - c) * k + c * m) % 4) * 4 + (y + c * k + (1 - c) * m) % 4


G_COPIES = 8 + 4 + 12 + 15


def gather_kernel(pack, sel, out, zbuf, send_sems, recv_sems):
    x, y, zh, c, zl = here()
    other = {"core": 1 - c}
    ahead, behind = {"zh": (zh + 1) % 4}, {"zh": (zh + 3) % 4}
    first_on, first_back = along(True, 1, x, y, c), along(True, 3, x, y, c)
    second_on, second_back = along(False, 1, x, y, c), along(False, 3, x, y, c)
    for device in (other, ahead, behind, first_on, first_back, second_on, second_back):
        greet(device)
    pl.semaphore_wait(pltpu.get_barrier_semaphore(), 7)
    go = Sender(send_sems, recv_sems)

    def slot(k):
        return pl.ds(pl.multiple_of((((zh + k) % 4) * 2 + c) * 32, 32), 32)

    zbuf[slot(0), :] = pack[...]
    mine = zbuf.at[slot(0), :]
    from_behind = go(pack, mine, ahead)
    from_ahead = go(pack, mine, behind)
    shared = [go(pack, mine, other)]
    from_behind.wait_recv()
    held = zbuf.at[slot(3), 0:384]
    part_on = go(held, held, ahead)
    held = zbuf.at[slot(3), :]
    shared.append(go(held, held, other))
    from_ahead.wait_recv()
    held = zbuf.at[slot(1), 384:640]
    part_back = go(held, held, behind)
    held = zbuf.at[slot(1), :]
    shared.append(go(held, held, other))
    part_on.wait_recv()
    part_back.wait_recv()
    held = zbuf.at[slot(2), :]
    shared.append(go(held, held, other))
    for copy in shared:
        copy.wait_recv()

    rows = jnp.dot(sel[...], zbuf[...], preferred_element_type=F32).astype(BF16)
    at = x * 4 + y
    out[0, at] = rows[0:80]
    out[1, at] = rows[80:160]

    def held_block(k, m):
        return out.at[c, block(k, m, x, y, c)]

    crossed = []

    def pass_on(k):
        b = held_block(k, 0)
        return (go(b, b, second_on), go(b, b, second_back))

    def across(k, m):
        b = held_block(k, m)
        crossed.append(go(b, b, other))

    own = held_block(0, 0)
    from_back = go(own, own, first_on)
    from_on = go(own, own, first_back)
    seconds = {0: pass_on(0)}
    from_back.wait_recv()
    b = out.at[c, block(3, 0, x, y, c), :, 0:384]
    part_on = go(b, b, first_on)
    seconds[3] = pass_on(3)
    across(3, 0)
    from_on.wait_recv()
    b = out.at[c, block(1, 0, x, y, c), :, 384:640]
    part_back = go(b, b, first_back)
    seconds[1] = pass_on(1)
    across(1, 0)
    relays = []
    for k in (0, 3, 1, 2):
        if k == 2:
            part_on.wait_recv()
            part_back.wait_recv()
            seconds[2] = pass_on(2)
            across(2, 0)
        seconds[k][0].wait_recv()
        if k in (0, 1):
            b = held_block(k, 3)
            relays.append((k, go(b, b, second_on)))
        across(k, 3)
        seconds[k][1].wait_recv()
        if k in (3, 2):
            b = held_block(k, 1)
            relays.append((k, go(b, b, second_back)))
        across(k, 1)
    for k, copy in relays:
        copy.wait_recv()
        across(k, 2)
    for copy in crossed:
        copy.wait_recv()
    go.finish()


def gather(pack, sel):
    return pl.pallas_call(
        gather_kernel,
        out_shape=jax.ShapeDtypeStruct((2, 16, 80, 640), BF16),
        in_specs=[VMEM, VMEM],
        out_specs=VMEM,
        scratch_shapes=[
            pltpu.VMEM((256, 640), BF16),
            pltpu.SemaphoreType.DMA((G_COPIES,)),
            pltpu.SemaphoreType.DMA((G_COPIES,)),
        ],
        compiler_params=pltpu.CompilerParams(collective_id=0, has_side_effects=True),
        name="gather",
    )(pack, sel)


def contract_last(left, right):
    return lax.dot_general(left, right, (((1,), (1,)), ((), ())), preferred_element_type=F32)


def contract_first(left, right):
    return lax.dot_general(left, right, (((0,), (0,)), ((), ())), preferred_element_type=F32)


def compute_kernel(
    s_in, t_in, vecs, feats, feats_t, w, grads, sums, emb, emb_grad, w_out, normed_s, mix_s, hidden_s, grad_s
):
    lane = lax.broadcasted_iota(jnp.int32, (1, 384), 1)
    in_s, in_t = lane < 320, lane >= 64
    for i in range(8):
        a = w[1, 2 * i].astype(F32)[0:40]
        b = w[1, 2 * i + 1].astype(F32)[0:40]
        w_out[80 * i : 80 * i + 80, :] = jnp.concatenate([a, b], axis=0).astype(BF16)
    rest = w[1].reshape(1280, 640)
    emb[...] = jnp.dot(feats[...], rest, preferred_element_type=F32)

    def forward(tokens, shift, gain, bias, inside, lanes):
        summed = jnp.where(inside, tokens.astype(F32) + shift, 0.0)
        mean = jnp.sum(summed, axis=1, keepdims=True) / 320
        center = jnp.where(inside, summed - mean, 0.0)
        inv_std = lax.rsqrt(jnp.sum(center * center, axis=1, keepdims=True) / 320 + 1e-05)
        normed = center * inv_std
        normed_b = (normed * gain + bias).astype(BF16)
        mixed = contract_last(normed_b, w[0, :, :, lanes].reshape(1280, 384))
        gate, up = mixed[:, :640], mixed[:, 640:]
        tangent = jnp.tanh(0.7978845608 * (gate + 0.044715 * gate * gate * gate))
        gelu = 0.5 * gate * (1.0 + tangent)
        hidden = (gelu * up).astype(BF16)
        out = summed + jnp.dot(hidden, w_out[:, lanes], preferred_element_type=F32)
        return out, normed, inv_std, normed_b, gate, up, tangent, gelu, hidden

    sums[...] = jnp.zeros_like(sums)

    def one_sample(s, _):
        rows = pl.ds(pl.multiple_of(s * 256, 256), 256)
        zeros = jnp.zeros((256, 64), BF16)
        t = t_in[rows, :]
        tokens_t = jnp.concatenate([zeros, t[:, 256:320], t[:, 0:256]], axis=1)
        out_t = forward(
            tokens_t, emb[pl.ds(2 + s, 1), 256:640], vecs[2:3, :], vecs[3:4, :], in_t, slice(256, 640)
        )[0]
        tokens_s = jnp.concatenate([s_in[rows, :], zeros], axis=1)
        gain = vecs[0:1, :]
        out_s, normed, inv_std, normed_b, gate, up, tangent, gelu, hidden = forward(
            tokens_s, emb[pl.ds(s, 1), 0:384], gain, vecs[1:2, :], in_s, slice(0, 384)
        )
        turned = jnp.concatenate(
            [out_t[:, 128:384], pltpu.roll(out_t[:, 0:128], 64, axis=1)], axis=1
        )
        grad_y = jnp.where(in_s, (out_s - turned) / 512, 0.0)
        grad_yb = grad_y.astype(BF16)
        grad_h = contract_last(grad_yb, w_out[:, 0:384])
        slope = 0.5 * (1.0 + tangent) + 0.5 * gate * (1.0 - tangent * tangent) * 0.7978845608 * (
            1.0 + 0.134145 * gate * gate
        )
        grad_mix = jnp.concatenate(
            [(grad_h * up * slope).astype(BF16), (grad_h * gelu).astype(BF16)], axis=1
        )
        grad_z = jnp.dot(grad_mix, w[0, :, :, 0:384].reshape(1280, 384), preferred_element_type=F32)
        grad_z = jnp.where(in_s, grad_z, 0.0)
        sums[0, 0:1, :] += jnp.sum(grad_z * normed, axis=0, keepdims=True)
        sums[1, 0:1, :] += jnp.sum(grad_z, axis=0, keepdims=True)
        grad_n = grad_z * gain
        mean_n = jnp.sum(grad_n, axis=1, keepdims=True) / 320
        mean_nn = jnp.sum(grad_n * normed, axis=1, keepdims=True) / 320
        grad_sum = grad_y + inv_std * (grad_n - mean_n - normed * mean_nn)
        grad_sum = jnp.where(in_s, grad_sum, 0.0)
        emb_grad[pl.ds(s, 1), :] = jnp.sum(grad_sum, axis=0, keepdims=True)
        normed_s[rows, :] = normed_b
        mix_s[rows, :] = grad_mix
        hidden_s[rows, :] = hidden
        grad_s[rows, :] = grad_yb
        return 0

    lax.fori_loop(0, 2, one_sample, 0)
    full_in = contract_first(mix_s[...], normed_s[...])
    grads[0] = full_in.astype(BF16).reshape(16, 80, 384)
    full_out = contract_first(hidden_s[...], grad_s[...])
    full_time = feats_t[:, 0:1] * emb_grad[0:1, :] + feats_t[:, 1:2] * emb_grad[1:2, :]
    for b in range(16):
        r = slice(40 * b, 40 * b + 40)
        grads[1, b] = jnp.concatenate([full_out[r], full_time[r]], axis=0).astype(BF16)


def compute(s_in, t_in, vecs, feats, feats_t, w):
    return pl.pallas_call(
        compute_kernel,
        out_shape=(
            jax.ShapeDtypeStruct((2, 16, 80, 384), BF16),
            jax.ShapeDtypeStruct((2, 8, 384), F32),
        ),
        in_specs=[VMEM] * 6,
        out_specs=(VMEM, VMEM),
        scratch_shapes=[
            pltpu.VMEM((8, 640), F32),
            pltpu.VMEM((8, 384), F32),
            pltpu.VMEM((640, 640), BF16),
            pltpu.VMEM((512, 384), BF16),
            pltpu.VMEM((512, 1280), BF16),
            pltpu.VMEM((512, 640), BF16),
            pltpu.VMEM((512, 384), BF16),
        ],
        compiler_params=pltpu.CompilerParams(vmem_limit_bytes=60 * 2**20),
        name="step",
    )(s_in, t_in, vecs, feats, feats_t, w)


R_COPIES = 17 + 4 + 8 + 3 + 2 + 2 + 3 + 6


def reduce_kernel(
    grads, sums, spread, out, total, part, acc, early, from_back, from_on, mids, early_2, back_2, on_2,
    zblk, quarters, fin, vd, va, vb, vz, vfin, vown, owned, send_sems, recv_sems, far_send, far_recv,
):
    x, y, zh, c, zl = here()
    other = {"core": 1 - c}
    first_on, first_back = along(True, 1, x, y, c), along(True, 3, x, y, c)
    second_on, second_back = along(False, 1, x, y, c), along(False, 3, x, y, c)
    first_far, second_far = along(True, 2, x, y, c), along(False, 2, x, y, c)
    rep_peers = [{"zl": (zl + k) % 4} for k in (1, 2, 3)]
    near = [other, first_on, first_back, first_far, second_on, second_back, second_far] + rep_peers
    for device in near:
        greet(device)
    for h in range(4):
        for k in range(2):
            itself = (zl == zh) & (h == zh) & (k == c)

            @pl.when(jnp.logical_not(itself))
            def _():
                greet({"zh": h, "zl": zh, "core": k})

    barrier = pltpu.get_barrier_semaphore()
    pl.semaphore_wait(barrier, jnp.where(zl == zh, len(near) + 7, len(near) + 8))

    go = Sender(send_sems, recv_sems)
    pairs = [(k, m) for k in (2, 1, 3, 0) for m in range(4)]
    crossed = {}
    for k, m in pairs:
        b = block(k, m, x, y, 1 - c)
        crossed[k, m] = go(grads.at[1 - c, b], part.at[k * 4 + m], other)
    vec_in = go(sums.at[1 - c], vd, other)

    def local(k, m):
        crossed[k, m].wait_recv()
        b = block(k, m, x, y, c)
        return grads[c, b].astype(F32) + part[k * 4 + m].astype(F32)

    relay = {}
    for m in range(4):
        acc[8 + m] = local(2, m).astype(BF16)
        relay[m] = go(acc.at[8 + m], early.at[m], first_on if m < 2 else first_back)
    arrive_back, arrive_on = {}, {}
    for m in (2, 3):
        acc[4 + m] = local(1, m).astype(BF16)
        arrive_back[m] = go(acc.at[4 + m], from_back.at[m], first_on)
    for m in (0, 1):
        acc[12 + m] = local(3, m).astype(BF16)
        arrive_on[m] = go(acc.at[12 + m], from_on.at[m], first_back)

    vec_in.wait_recv()
    own = jnp.where(c == 0, x, y)
    va[own] = sums[c] + vd[...]
    vown[0] = va[own]
    vec_a = [go(vown.at[0], va.at[own], along(True, k, x, y, c)) for k in (1, 2, 3)]

    for m in (0, 1):
        mine = local(1, m)
        relay[m].wait_recv()
        acc[4 + m] = (mine + early[m].astype(F32)).astype(BF16)
        arrive_back[m] = go(acc.at[4 + m], from_back.at[m], first_on)
    for m in (2, 3):
        mine = local(3, m)
        relay[m].wait_recv()
        acc[12 + m] = (mine + early[m].astype(F32)).astype(BF16)
        arrive_on[m] = go(acc.at[12 + m], from_on.at[m], first_back)

    for copy in vec_a:
        copy.wait_recv()
    own_2 = jnp.where(c == 0, y, x)
    vb[own_2] = ((va[0] + va[1]) + va[2]) + va[3]
    vown[1] = vb[own_2]
    vec_b = [go(vown.at[1], vb.at[own_2], along(False, k, x, y, c)) for k in (1, 2, 3)]

    def first_sum(m):
        mine = local(0, m)
        arrive_back[m].wait_recv()
        arrive_on[m].wait_recv()
        return mine + from_back[m].astype(F32) + from_on[m].astype(F32)

    mids[2] = first_sum(2).astype(BF16)
    up = go(mids.at[2, 0:48], early_2.at[0:48], second_on)
    down = go(mids.at[2, 48:80], early_2.at[48:80], second_back)
    mine_1, mine_3 = first_sum(1), first_sum(3)
    up.wait_recv()
    mids[1, 0:48] = (mine_1[0:48] + early_2[0:48].astype(F32)).astype(BF16)
    mids[1, 48:80] = mine_1[48:80].astype(BF16)
    last_back = go(mids.at[1], back_2, second_on)
    down.wait_recv()
    mids[3, 0:48] = mine_3[0:48].astype(BF16)
    mids[3, 48:80] = (mine_3[48:80] + early_2[48:80].astype(F32)).astype(BF16)
    last_on = go(mids.at[3], on_2, second_back)
    mine_0 = first_sum(0)

    for copy in vec_b:
        copy.wait_recv()
    vz[zl] = ((vb[0] + vb[1]) + vb[2]) + vb[3]
    vown[2] = vz[zl]
    vec_z = [go(vown.at[2], vz.at[zl], device) for device in rep_peers]

    last_back.wait_recv()
    last_on.wait_recv()
    plane = (mine_0 + back_2[...].astype(F32) + on_2[...].astype(F32)).astype(BF16)
    zblk[...] = jnp.dot(spread[c], plane, preferred_element_type=F32).astype(BF16).reshape(8, 16, 384)
    quarters[zl] = zblk[pl.ds(2 * zl, 2)]
    rep_in = []
    for k in (1, 2, 3):
        j = (zl + k) % 4
        rep_in.append(go(zblk.at[pl.ds(2 * j, 2)], quarters.at[zl], {"zl": j}))
    for copy in rep_in:
        copy.wait_recv()
    q = [quarters[j].astype(F32) for j in range(4)]
    owned[...] = (((q[0] + q[1]) + q[2]) + q[3]).astype(BF16)
    for copy in vec_z:
        copy.wait_recv()
    vown[3] = ((vz[0] + vz[1]) + vz[2]) + vz[3]

    me = zh * 2 + c
    for j in range(4):
        for k in range(2):
            itself = (zl == zh) & (j == zl) & (k == c)
            at = j * 2 + k
            device = {"zh": zl, "zl": j, "core": k}

            @pl.when(jnp.logical_not(itself))
            def _():
                send(owned.at[k], fin.at[me], far_send.at[at], far_recv.at[me], device)
                send(vown.at[3], vfin.at[me], far_send.at[8 + at], far_recv.at[8 + me], device)

    @pl.when(zl == zh)
    def _():
        fin[me] = owned[c]
        vfin[me] = vown[3]

    def far(at, src, dst, recv):
        return pltpu.make_async_remote_copy(
            src_ref=src, dst_ref=dst, send_sem=far_send.at[at], recv_sem=far_recv.at[recv],
            device_id=other, device_id_type=pl.DeviceIdType.MESH,
        )

    for h in range(4):
        for k in range(2):
            at = h * 2 + k
            itself = (zl == zh) & (h == zh) & (k == c)

            @pl.when(jnp.logical_not(itself))
            def _():
                far(at, owned.at[0], fin.at[at], at).wait_recv()
                far(8 + at, vown.at[3], vfin.at[at], 8 + at).wait_recv()

    for k in range(2):
        f = [fin[2 * h + k].astype(F32) for h in range(4)]
        out[k] = ((f[0] + f[1]) + f[2]) + f[3]
        total[k] = ((vfin[k] + vfin[2 + k]) + vfin[4 + k]) + vfin[6 + k]
    go.finish()
    for j in range(4):
        for k in range(2):
            itself = (zl == zh) & (j == zl) & (k == c)
            at = j * 2 + k

            @pl.when(jnp.logical_not(itself))
            def _():
                far(at, owned.at[0], fin.at[at], at).wait_send()
                far(8 + at, vown.at[3], vfin.at[at], 8 + at).wait_send()


def reduce(grads, sums, spread):
    return pl.pallas_call(
        reduce_kernel,
        out_shape=(
            jax.ShapeDtypeStruct((2, 16, 384), F32),
            jax.ShapeDtypeStruct((2, 8, 384), F32),
        ),
        in_specs=[VMEM] * 3,
        out_specs=(VMEM, VMEM),
        scratch_shapes=[
            pltpu.VMEM((16, 80, 384), BF16),
            pltpu.VMEM((16, 80, 384), BF16),
            pltpu.VMEM((4, 80, 384), BF16),
            pltpu.VMEM((4, 80, 384), BF16),
            pltpu.VMEM((4, 80, 384), BF16),
            pltpu.VMEM((4, 80, 384), BF16),
            pltpu.VMEM((80, 384), BF16),
            pltpu.VMEM((80, 384), BF16),
            pltpu.VMEM((80, 384), BF16),
            pltpu.VMEM((8, 16, 384), BF16),
            pltpu.VMEM((4, 2, 16, 384), BF16),
            pltpu.VMEM((8, 16, 384), BF16),
            pltpu.VMEM((8, 384), F32),
            pltpu.VMEM((4, 8, 384), F32),
            pltpu.VMEM((4, 8, 384), F32),
            pltpu.VMEM((4, 8, 384), F32),
            pltpu.VMEM((8, 8, 384), F32),
            pltpu.VMEM((4, 8, 384), F32),
            pltpu.VMEM((2, 16, 384), BF16),
            pltpu.SemaphoreType.DMA((R_COPIES,)),
            pltpu.SemaphoreType.DMA((R_COPIES,)),
            pltpu.SemaphoreType.DMA((16,)),
            pltpu.SemaphoreType.DMA((16,)),
        ],
        compiler_params=pltpu.CompilerParams(collective_id=1, has_side_effects=True),
        name="reduce",
    )(grads, sums, spread)


def selection():
    sel = np.zeros((160, 256), np.float32)
    spread = np.zeros((2, 128, 80), np.float32)
    for d in range(8):
        for r in range(10):
            sel[d * 10 + r, d * 32 + r] = 1
            spread[0, d * 16 + r, d * 10 + r] = 1
        for r in range(5):
            sel[80 + d * 5 + r, d * 32 + 10 + r] = 1
            sel[120 + d * 5 + r, d * 32 + 15 + r] = 1
            spread[1, d * 16 + r, d * 5 + r] = 1
            spread[1, d * 16 + 5 + r, 40 + d * 5 + r] = 1
    return jnp.asarray(sel, BF16), jnp.asarray(spread, BF16)


def sinusoid(step_ids, width, order):
    half_width = width // 2
    frequency = jnp.exp(-math.log(10000.0) * (order % half_width).astype(F32) / half_width)
    angles = step_ids.astype(F32)[:, None] * frequency[None, :]
    wave = jnp.where(order[None, :] < half_width, jnp.cos(angles), jnp.sin(angles))
    return jax.nn.silu(wave)


def per_device(
    student_in, target_in, timesteps,
    student_win, student_wout, student_wtime, student_gain, student_bias,
    target_win, target_wout, target_wtime, target_gain, target_bias,
):
    sel, spread = selection()
    rows_s = jnp.concatenate([student_win, student_wout, student_wtime], axis=0)
    rows_t = jnp.concatenate([target_win, target_wout, target_wtime], axis=0)
    pack = jnp.concatenate([rows_s, rows_t[:, 256:], rows_t[:, :256]], axis=1).astype(BF16)
    pack = jnp.pad(pack, ((0, 12), (0, 0)))
    weights = gather(pack, sel)

    spot = jnp.arange(1280, dtype=jnp.int32)
    order = (spot // 80) * 40 + spot % 80 - 40
    steps = jnp.concatenate([timesteps, timesteps - SKIP])
    feats = jnp.where(spot[None, :] % 80 >= 40, sinusoid(steps, 640, order), 0.0)
    feats = jnp.pad(feats.astype(BF16), ((0, 4), (0, 0)))
    plain = sinusoid(timesteps, 640, jnp.arange(640, dtype=jnp.int32)).astype(BF16)
    feats_t = plain.astype(F32).T
    student = jnp.pad(jnp.stack([student_gain, student_bias]), ((0, 0), (0, 64)))
    target = jnp.stack([target_gain, target_bias])
    target = jnp.concatenate([jnp.zeros((2, 64), F32), target[:, 256:], target[:, :256]], axis=1)
    vecs = jnp.concatenate([student, target, jnp.zeros((4, 384), F32)], axis=0)
    grads, sums = compute(student_in, target_in, vecs, feats, feats_t, weights)
    owned, totals = reduce(grads, sums, spread)
    grad_win = owned[0, :10, :320]
    grad_wout = owned[1, :5, :320]
    grad_wtime = owned[1, 5:10, :320]
    grad_gain, grad_bias = totals[0, 0, :320], totals[1, 0, :320]

    def average(target_p, student_p, grad_p):
        return EMA_DECAY * target_p + (1.0 - EMA_DECAY) * (student_p - LEARN_RATE * grad_p)

    return (
        grad_win, grad_wout, grad_wtime, grad_gain, grad_bias,
        average(target_win, student_win, grad_win),
        average(target_wout, student_wout, grad_wout),
        average(target_wtime, student_wtime, grad_wtime),
        average(target_gain, student_gain, grad_gain),
        average(target_bias, student_bias, grad_bias),
    )


def solution(mesh):
    split = Mesh(mesh.devices.reshape(4, 4, 4, 2, 4), DP_REP)
    row, vec, tok = P(DP, None), P(), P(DP_REP, None)
    return jax.shard_map(
        per_device,
        mesh=split,
        in_specs=(tok, tok, P(DP_REP), row, row, row, vec, vec, row, row, row, vec, vec),
        out_specs=(row, row, row, vec, vec, row, row, row, vec, vec),
        check_vma=False,
    )
```
